32 devices in a mesh: rows: 8 (over z, x), width: 4 (over y, core).
Axes of the slice: x: 2, y: 2, z: 4, core: 2. Of those that a mesh axis runs over, the one named last changes fastest.
Arguments:
- w_gate: float32 [3072, 8192], P('rows', 'width'), may hold values from -0.15625 to 0.15625
- avg_gate: float32 [3072, 8192], P('rows', 'width'), may hold values from -0.109375 to 0.109375
- w_up: float32 [3072, 8192], P('rows', 'width'), may hold values from -0.15625 to 0.15625
- avg_up: float32 [3072, 8192], P('rows', 'width'), may hold values from -0.109375 to 0.109375
- norm_gain: float32 [3072], P('rows'), may hold values from 0.25 to 1.75
Outputs:
- serve_gate: bfloat16 [3072, 8192], P(None, 'width')
- serve_up: bfloat16 [3072, 8192], P(None, 'width')
- factor_gate: float32 [8192], P('width')
- factor_up: float32 [8192], P('width')
The draws below stay inside these ranges and needn't reach their ends.
All inputs are finite; a program needn't handle non-finite values. Where the reference program divides by a largest or mean magnitude, that divisor is 1e-20 or more.
Results may differ from the reference program's by a relative error of at most 0.001.
Values may be sent and summed in bfloat16 or wider, within the bound.
A program may use at most 128 MiB of HBM per device.

```python
import jax
import jax.numpy as jnp

D_MODEL = 3072
D_INNER = 8192


def with_spikes(drawn, rng, source, target, parts, factor):
    owner, partner = [(jnp.arange(drawn.shape[axis_at]) // (drawn.shape[axis_at] // parts)).reshape([-1 if axis == axis_at else 1 for axis in range(drawn.ndim)]) for axis_at in (source, target)]
    chosen = jax.random.permutation(rng, parts)[partner]
    strong = (owner == chosen) | (owner == (partner + parts // 2) % parts)
    return jnp.where(strong, factor * drawn, drawn)


def block_scale(stream_key, extent, shards, low, top_value):
    factor_of, own = 1.0, jax.random.fold_in(stream_key, 6)
    for axis_at, shards_of in shards:
        draws = jnp.exp(jax.random.uniform(jax.random.fold_in(own, axis_at), (shards_of,), jnp.float32, low / len(shards), top_value / len(shards)))
        factor_of = factor_of * jnp.repeat(draws, extent[axis_at] // shards_of).reshape([-1 if axis == axis_at else 1 for axis in range(len(extent))])
    return factor_of


def bell_draw(rng, shape, width, limit, split=(), kind=jnp.bfloat16):
    result = jax.random.normal(rng, shape, jnp.float32) * width
    if len(split) > 0:
        result = block_scale(rng, shape, split, -0.22, 0.18) * result
    return jnp.clip(result, min=-limit, max=limit).astype(kind)


def bell_draw_with(stream_key, extent, spread, reach, pieces, heavy, held_as=jnp.bfloat16):
    values = spread * jax.random.normal(stream_key, extent, jnp.float32)
    if pieces:
        values = values * block_scale(stream_key, extent, pieces, -0.22, 0.18)
    return jnp.clip(with_spikes(values, jax.random.fold_in(stream_key, 3), *heavy), -reach, reach).astype(held_as)


def setup_inputs(seed: int = 0) -> dict:
    keys = jax.random.split(jax.random.key(seed), 6)
    return {
        "w_gate": bell_draw_with(keys[0], (D_MODEL, D_INNER), D_MODEL ** -0.5, 0.15625, ((0, 8), (1, 4)), (0, 1, 8, 2.0), jnp.float32),
        "avg_gate": bell_draw(keys[1], (D_MODEL, D_INNER), D_MODEL ** -0.5, 0.109375, ((0, 8), (1, 4)), jnp.float32),
        "w_up": bell_draw_with(keys[2], (D_MODEL, D_INNER), D_MODEL ** -0.5, 0.15625, ((0, 8), (1, 4)), (0, 1, 8, 2.0), jnp.float32),
        "avg_up": bell_draw(keys[3], (D_MODEL, D_INNER), D_MODEL ** -0.5, 0.109375, ((0, 8), (1, 4)), jnp.float32),
        "norm_gain": jnp.clip(1.0 + 0.15 * jax.random.normal(keys[4], (D_MODEL,), jnp.float32), 0.25, 1.75),
    }


keep_rate = 0.7


def reference(w_gate, avg_gate, w_up, avg_up, norm_gain):
    fresh_gate = keep_rate * avg_gate + (1.0 - keep_rate) * w_gate
    fresh_up = keep_rate * avg_up + (1.0 - keep_rate) * w_up
    fresh_gained_gate = fresh_gate * norm_gain[:, None]
    fresh_gained_up = fresh_up * norm_gain[:, None]
    factor_gate = jnp.max(jnp.abs(fresh_gained_gate), axis=0)
    serve_gate = (fresh_gained_gate / factor_gate).astype(jnp.bfloat16)
    factor_up = jnp.max(jnp.abs(fresh_gained_up), axis=0)
    serve_up = (fresh_gained_up / factor_up).astype(jnp.bfloat16)
    return serve_gate, serve_up, factor_gate, factor_up
```

```python
import functools

import jax
import jax.numpy as jnp
from jax import lax
from jax.experimental import pallas as pl
from jax.experimental.pallas import tpu as pltpu
from jax.sharding import PartitionSpec as P

keep_rate = 0.7
MESH = pl.DeviceIdType.MESH
CHUNKS = 4
VMEM_LIMIT = 36 * 2**20


def ring_place(r, n):
    if n % 2:
        return r
    x, z = r % 2, r // 2
    return z + x * (n - 1 - 2 * z)


def ring_row(p, n):
    if n % 2:
        return p
    half = n // 2
    x, k = p // half, p % half
    return 2 * (k + x * (half - 1 - 2 * k)) + x


def serve_kernel(
    n, chunks, gain_ref, wg_ref, ag_ref, wu_ref, au_ref, go_ref, uo_ref, fg_ref, fu_ref,
    w_in, fresh, gains, part, got, in_sem, max_send, max_recv, send_sem, recv_sem,
):
    me = lax.axis_index("rows")
    place = ring_place(me, n)
    nxt = ring_row((place + 1) % n, n)
    prv = ring_row((place + n - 1) % n, n)
    rows, columns = wg_ref.shape
    size = rows // chunks
    outs, to = (go_ref, uo_ref), (nxt, prv)

    loads = []
    for c in range(chunks):
        at = pl.ds(c * size, size)
        for k, (w_ref, avg_ref) in enumerate(((wg_ref, ag_ref), (wu_ref, au_ref))):
            for j, (src, dst) in enumerate(((w_ref, w_in), (avg_ref, fresh))):
                load = pltpu.make_async_copy(src.at[at], dst.at[k, at], in_sem.at[c, k, j])
                load.start()
                loads.append(load)

    barrier = pltpu.get_barrier_semaphore()
    for d in range(1, n):
        pl.semaphore_signal(barrier, inc=1, device_id={"rows": (me + d) % n}, device_id_type=MESH)

    for first in range(0, rows, 128):
        count = min(128, rows - first)
        line = gain_ref[first : first + count].reshape(1, count)
        gains[first : first + count, :] = jnp.broadcast_to(line, (128, count)).T

    tops = [jnp.zeros((8, columns), jnp.float32)] * 2
    for c in range(chunks):
        for k in range(2):
            loads[(c * 2 + k) * 2].wait()
            loads[(c * 2 + k) * 2 + 1].wait()

            def blend(i, top):
                at = pl.ds(pl.multiple_of(c * size + i * 8, 8), 8)
                gain = jnp.tile(gains[at, :], (1, columns // 128))
                value = (keep_rate * fresh[k, at, :] + (1.0 - keep_rate) * w_in[k, at, :]) * gain
                fresh[k, at, :] = value
                return jnp.maximum(top, jnp.abs(value))

            tops[k] = lax.fori_loop(0, size // 8, blend, tops[k])
    for k in range(2):
        part[k : k + 1, :] = jnp.max(tops[k], axis=0, keepdims=True)

    pl.semaphore_wait(barrier, n - 1)
    copies = []
    for d in range(1, n):
        copy = pltpu.make_async_remote_copy(
            src_ref=part,
            dst_ref=got.at[d - 1],
            send_sem=max_send.at[d - 1],
            recv_sem=max_recv.at[d - 1],
            device_id={"rows": (me + d) % n},
            device_id_type=MESH,
        )
        copy.start()
        copies.append(copy)
    for copy in copies:
        copy.wait()
    factor = jnp.maximum(part[...], jnp.max(got[...], axis=0))
    fg_ref[...] = factor[0:1]
    fu_ref[...] = factor[1:2]
    scale = 1.0 / factor

    def here(turn, c):
        owner = ring_row((place + turn) % n, n)
        return pl.ds(pl.multiple_of(owner * rows + c * size, size), size)

    def send(way, step, c):
        at = here((n - step) if way == 0 else step, c)
        return pltpu.make_async_remote_copy(
            src_ref=outs[way].at[at],
            dst_ref=outs[way].at[at],
            send_sem=send_sem.at[way, step, c],
            recv_sem=recv_sem.at[way, step, c],
            device_id={"rows": to[way]},
            device_id_type=MESH,
        )

    def landed(way, step, c):
        at = here((n - step - 1) if way == 0 else (step + 1), c)
        pltpu.make_async_remote_copy(
            src_ref=outs[way].at[at],
            dst_ref=outs[way].at[at],
            send_sem=send_sem.at[way, step, c],
            recv_sem=recv_sem.at[way, step, c],
            device_id={"rows": to[way]},
            device_id_type=MESH,
        ).wait_recv()

    for c in range(chunks + 1):
        for way in range(2):
            if c < chunks:
                by = jnp.broadcast_to(scale[way : way + 1, :], (16, columns))

                @pl.loop(0, size // 16)
                def _(i):
                    at = pl.ds(pl.multiple_of(c * size + i * 16, 16), 16)
                    to_at = pl.ds(pl.multiple_of(me * rows + c * size + i * 16, 16), 16)
                    outs[way][to_at, :] = (fresh[way, at, :] * by).astype(jnp.bfloat16)

            if c:
                send(way, 0, c - 1).start()

    @pl.loop(1, n - 1)
    def _(step):
        for c in range(chunks):
            for way in range(2):
                landed(way, step - 1, c)
                send(way, step, c).start()

    for c in range(chunks):
        for way in range(2):
            landed(way, n - 2, c)

    for c in range(chunks):
        for way in range(2):
            send(way, 0, c).wait_send()

    @pl.loop(1, n - 1)
    def _(step):
        for c in range(chunks):
            for way in range(2):
                send(way, step, c).wait_send()


def serve(w_gate, avg_gate, w_up, avg_up, norm_gain, n):
    rows, columns = w_gate.shape
    chunks = CHUNKS
    while rows % (16 * chunks):
        chunks -= 1
    whole = pltpu.VMEM((n * rows, columns), jnp.bfloat16)
    line = jax.ShapeDtypeStruct((1, columns), jnp.float32)
    anywhere = pl.BlockSpec(memory_space=pl.ANY)
    near = pl.BlockSpec(memory_space=pltpu.VMEM)
    return pl.pallas_call(
        functools.partial(serve_kernel, n, chunks),
        out_shape=(whole, whole, line, line),
        in_specs=[near] + [anywhere] * 4,
        out_specs=(near, near, near, near),
        scratch_shapes=[
            pltpu.VMEM((2, rows, columns), jnp.float32),
            pltpu.VMEM((2, rows, columns), jnp.float32),
            pltpu.VMEM((rows, 128), jnp.float32),
            pltpu.VMEM((2, columns), jnp.float32),
            pltpu.VMEM((n - 1, 2, columns), jnp.float32),
            pltpu.SemaphoreType.DMA((chunks, 2, 2)),
            pltpu.SemaphoreType.DMA((n - 1,)),
            pltpu.SemaphoreType.DMA((n - 1,)),
            pltpu.SemaphoreType.DMA((2, n - 1, chunks)),
            pltpu.SemaphoreType.DMA((2, n - 1, chunks)),
        ],
        compiler_params=pltpu.CompilerParams(
            collective_id=0, has_side_effects=True, vmem_limit_bytes=VMEM_LIMIT
        ),
        name="serve",
    )(norm_gain, w_gate, avg_gate, w_up, avg_up)


def keep_kernel(parts, gate_ref, up_ref, go_ref, uo_ref, sem):
    size = gate_ref.shape[0] // parts
    copies = []
    for c in range(parts):
        at = pl.ds(c * size, size)
        for k, (src, dst) in enumerate(((gate_ref, go_ref), (up_ref, uo_ref))):
            copy = pltpu.make_async_copy(src.at[at], dst.at[at], sem.at[k, c])
            copy.start()
            copies.append(copy)
    for copy in copies:
        copy.wait()


def keep(gate, up):
    parts = 8
    whole = jax.ShapeDtypeStruct(gate.shape, gate.dtype)
    near = pl.BlockSpec(memory_space=pltpu.VMEM)
    anywhere = pl.BlockSpec(memory_space=pl.ANY)
    return pl.pallas_call(
        functools.partial(keep_kernel, parts),
        out_shape=(whole, whole),
        in_specs=[near] * 2,
        out_specs=(anywhere,) * 2,
        scratch_shapes=[pltpu.SemaphoreType.DMA((2, parts))],
        compiler_params=pltpu.CompilerParams(vmem_limit_bytes=2**20),
        name="keep",
    )(gate, up)


def local(n, w_gate, avg_gate, w_up, avg_up, norm_gain):
    serve_gate, serve_up, factor_gate, factor_up = serve(w_gate, avg_gate, w_up, avg_up, norm_gain, n)
    serve_gate, serve_up = keep(serve_gate, serve_up)
    return (serve_gate, serve_up, factor_gate[0], factor_up[0])


def solution(mesh):
    placed = (P("rows", "width"),) * 4 + (P("rows"),)
    return jax.shard_map(
        functools.partial(local, mesh.shape["rows"]),
        mesh=mesh,
        in_specs=placed,
        out_specs=(P(None, "width"), P(None, "width"), P("width"), P("width")),
        check_vma=False,
    )
```

```python
import functools

import jax
import jax.numpy as jnp
from jax import lax
from jax.experimental import pallas as pl
from jax.experimental.pallas import tpu as pltpu
from jax.sharding import PartitionSpec as P

keep_rate = 0.7
MESH = pl.DeviceIdType.MESH
PARTS = 2
TAIL = 1
SPLIT = 8
EARLY = 16
KEEP = 8
VMEM_LIMIT = 36 * 2**20


def ring_place(r, n):
    if n % 2:
        return r
    x, z = r % 2, r // 2
    return z + x * (n - 1 - 2 * z)


def ring_row(p, n):
    if n % 2:
        return p
    half = n // 2
    x, k = p // half, p % half
    return 2 * (k + x * (half - 1 - 2 * k)) + x


def serve_kernel(
    n, parts, gain_ref, wg_ref, ag_ref, wu_ref, au_ref,
    go_ref, uo_ref, fg_ref, fu_ref, gt_ref, ut_ref,
    w_in, fresh, early, gains, part, got,
    in_sem, max_send, max_recv, early_send, early_recv, send_sem, recv_sem, tail_sem,
):
    me = lax.axis_index("rows")
    place = ring_place(me, n)
    nxt = ring_row((place + 1) % n, n)
    prv = ring_row((place + n - 1) % n, n)
    rows, columns = wg_ref.shape
    half = rows // 2
    size = half // parts
    chunks = 2 * parts
    outs, to = (go_ref, uo_ref), (nxt, prv)
    ins = ((wg_ref, ag_ref), (wu_ref, au_ref))

    spans = [(0, way * half, size) for way in range(2)]
    spans += [(0, way * half + size, half - size) for way in range(2)]
    spans += [(1, way * half, half) for way in range(2)]
    for s, (k, first, count) in enumerate(spans):
        at = pl.ds(first, count)
        for j, dst in enumerate((w_in, fresh)):
            load = pltpu.make_async_copy(ins[k][j].at[at], dst.at[k, at], in_sem.at[s])
            load.start()

    barrier = pltpu.get_barrier_semaphore()
    for d in range(1, n):
        pl.semaphore_signal(barrier, inc=1, device_id={"rows": (me + d) % n}, device_id_type=MESH)

    for first in range(0, rows, 128):
        count = min(128, rows - first)
        line = gain_ref[first : first + count].reshape(1, count)
        gains[first : first + count, :] = jnp.broadcast_to(line, (128, count)).T

    def blend(s, top):
        k, first, count = spans[s]
        both = fresh.at[k, pl.ds(0, 2 * count)]
        pltpu.make_async_copy(both, both, in_sem.at[s]).wait()

        def body(i, top):
            at = pl.ds(pl.multiple_of(first + i * 8, 8), 8)
            gain = jnp.tile(gains[at, :], (1, columns // 128))
            value = (keep_rate * fresh[k, at, :] + (1.0 - keep_rate) * w_in[k, at, :]) * gain
            fresh[k, at, :] = value
            return jnp.maximum(top, jnp.abs(value))

        return lax.fori_loop(0, count // 8, body, top)

    cuts = ((0, SPLIT), (SPLIT, EARLY))

    def ahead(way, b):
        first, end = cuts[b]
        return pltpu.make_async_remote_copy(
            src_ref=fresh.at[0, pl.ds(way * half + first, end - first)],
            dst_ref=early.at[way, pl.ds(first, end - first)],
            send_sem=early_send.at[way],
            recv_sem=early_recv.at[way],
            device_id={"rows": to[way]},
            device_id_type=MESH,
        )

    def spread(k, top):
        part[k] = jnp.max(top, axis=0, keepdims=True)
        for d in range(1, n):
            pltpu.make_async_remote_copy(
                src_ref=part.at[k],
                dst_ref=got.at[k, d - 1],
                send_sem=max_send.at[k],
                recv_sem=max_recv.at[k],
                device_id={"rows": (me + d) % n},
                device_id_type=MESH,
            ).start()

    def drained(ref, sem):
        pltpu.make_async_copy(ref, ref, sem).wait()

    def gather(k, out):
        drained(got.at[k], max_recv.at[k])
        factor = part[k]
        for d in range(n - 1):
            factor = jnp.maximum(factor, got[k, d])
        out[...] = factor
        return 1.0 / factor

    top = jnp.zeros((8, columns), jnp.float32)
    top = blend(0, top)
    top = blend(1, top)
    pl.semaphore_wait(barrier, n - 1)
    for way in range(2):
        ahead(way, 0).start()
    top = blend(2, top)
    top = blend(3, top)
    spread(0, top)
    for way in range(2):
        ahead(way, 1).start()
    top = jnp.zeros((8, columns), jnp.float32)
    top = blend(4, top)
    top = blend(5, top)
    spread(1, top)

    def block(turn):
        return ring_row((place + turn) % n, n) * rows

    def turn_out(way, step):
        return (n - step) if way == 0 else step

    def turn_in(way, step):
        return (n - step - 1) if way == 0 else (step + 1)

    def moved(way, step, q, turn, skip=0):
        k, first = q // parts, way * half + (q % parts) * size + skip
        at = outs[k].at[pl.ds(pl.multiple_of(block(turn) + first, 16), size - skip)]
        return pltpu.make_async_remote_copy(
            src_ref=at,
            dst_ref=at,
            send_sem=send_sem.at[way],
            recv_sem=recv_sem.at[way, step, q],
            device_id={"rows": to[way]},
            device_id_type=MESH,
        )

    def send(way, step, q, skip=0):
        return moved(way, step, q, turn_out(way, step), skip)

    def landed(way, step, q, skip=0):
        moved(way, step, q, turn_in(way, step), skip).wait_recv()

    def narrow(k, scale, load, first, count, base):
        by = jnp.broadcast_to(scale, (16, columns))

        @pl.loop(0, count // 16)
        def _(i):
            to_at = pl.ds(pl.multiple_of(base + i * 16, 16), 16)
            outs[k][to_at, :] = (load(pl.ds(pl.multiple_of(first + i * 16, 16), 16)) * by).astype(jnp.bfloat16)

    pending = []
    for k in range(2):
        scale = gather(k, (fg_ref, fu_ref)[k])
        if k == 0:
            gate_scale = scale
        for p in range(parts):
            for way in range(2):
                skip = EARLY if k == 0 and p == 0 else 0
                first = way * half + p * size + skip
                if skip < size:
                    narrow(k, scale, lambda at: fresh[k, at, :], first, size - skip, block(0) + first)
                    pending.append(send(way, 0, k * parts + p, skip))
                if len(pending) > 1:
                    pending.pop(0).start()
    pending.pop(0).start()
    for way in range(2):
        drained(early.at[way], early_recv.at[way])
        narrow(0, gate_scale, lambda at: early[way, at, :], 0, EARLY, block(turn_in(way, 0)) + way * half)
    for way in range(2):
        narrow(0, gate_scale, lambda at: fresh[0, at, :], way * half, EARLY, block(0) + way * half)

    skips = [EARLY] + [0] * (chunks - 1)
    for q in range(chunks):
        for way in range(2):
            if skips[q] < size:
                landed(way, 0, q, skips[q])
            send(way, 1, q).start()

    @pl.loop(2, n - 2)
    def _(step):
        for q in range(chunks):
            for way in range(2):
                landed(way, step - 1, q)
                send(way, step, q).start()

    last = n - 2
    for q in range(TAIL):
        for way in range(2):
            landed(way, last - 1, q)
    tails = []
    for way, ref in enumerate((gt_ref, ut_ref)):
        at = pl.ds(pl.multiple_of(block(turn_out(way, last)) + way * half, 16), TAIL * size)
        copy = pltpu.make_async_copy(go_ref.at[at], ref, tail_sem.at[way])
        copy.start()
        tails.append(copy)
    for q in range(TAIL, chunks):
        for way in range(2):
            landed(way, last - 1, q)
            send(way, last, q).start()
    for copy in tails:
        copy.wait()

    for q in range(TAIL, chunks):
        for way in range(2):
            landed(way, last, q)
    for way in range(2):
        drained(early.at[way], early_send.at[way])
        drained(got.at[way], max_send.at[way])
        sent = go_ref.at[pl.ds(0, (n - 1) * rows - EARLY - TAIL * size)]
        drained(sent, send_sem.at[way])


def serve(w_gate, avg_gate, w_up, avg_up, norm_gain, n):
    rows, columns = w_gate.shape
    half = rows // 2
    parts = PARTS
    while half % (16 * parts):
        parts -= 1
    size = half // parts
    whole = pltpu.VMEM((n * rows, columns), jnp.bfloat16)
    tail = pltpu.HBM((TAIL * size, columns), jnp.bfloat16)
    line = pltpu.VMEM((1, columns), jnp.float32)
    anywhere = pl.BlockSpec(memory_space=pl.ANY)
    near = pl.BlockSpec(memory_space=pltpu.VMEM)
    return pl.pallas_call(
        functools.partial(serve_kernel, n, parts),
        out_shape=(whole, whole, line, line, tail, tail),
        in_specs=[near] + [anywhere] * 4,
        out_specs=(near, near, near, near, anywhere, anywhere),
        scratch_shapes=[
            pltpu.VMEM((2, rows, columns), jnp.float32),
            pltpu.VMEM((2, rows, columns), jnp.float32),
            pltpu.VMEM((2, EARLY, columns), jnp.float32),
            pltpu.VMEM((rows, 128), jnp.float32),
            pltpu.VMEM((2, 1, columns), jnp.float32),
            pltpu.VMEM((2, n - 1, 1, columns), jnp.float32),
            pltpu.SemaphoreType.DMA((6,)),
            pltpu.SemaphoreType.DMA((2,)),
            pltpu.SemaphoreType.DMA((2,)),
            pltpu.SemaphoreType.DMA((2,)),
            pltpu.SemaphoreType.DMA((2,)),
            pltpu.SemaphoreType.DMA((2,)),
            pltpu.SemaphoreType.DMA((2, n - 1, 2 * parts)),
            pltpu.SemaphoreType.DMA((2,)),
        ],
        compiler_params=pltpu.CompilerParams(
            collective_id=0, has_side_effects=True, vmem_limit_bytes=VMEM_LIMIT
        ),
        name="serve",
    )(norm_gain, w_gate, avg_gate, w_up, avg_up)


def keep_kernel(parts, gate_ref, up_ref, fg_ref, fu_ref, go_ref, uo_ref, fgo_ref, fuo_ref, lines, sem, line_sem):
    size = gate_ref.shape[0] // parts
    for c in range(parts):
        at = pl.ds(c * size, size)
        for k, (src, dst) in enumerate(((gate_ref, go_ref), (up_ref, uo_ref))):
            pltpu.make_async_copy(src.at[at], dst.at[at], sem.at[k]).start()
    for k, (src, dst) in enumerate(((fg_ref, fgo_ref), (fu_ref, fuo_ref))):
        lines[k][...] = src[0]
        pltpu.make_async_copy(lines[k], dst, line_sem.at[k]).start()
    for k, (ref, out, line) in enumerate(((gate_ref, go_ref, fgo_ref), (up_ref, uo_ref, fuo_ref))):
        pltpu.make_async_copy(ref, out, sem.at[k]).wait()
        pltpu.make_async_copy(lines[k], line, line_sem.at[k]).wait()


def keep(gate, up, factor_gate, factor_up):
    parts = KEEP
    columns = gate.shape[1]
    whole = jax.ShapeDtypeStruct(gate.shape, gate.dtype)
    line = jax.ShapeDtypeStruct((columns,), factor_gate.dtype)
    near = pl.BlockSpec(memory_space=pltpu.VMEM)
    anywhere = pl.BlockSpec(memory_space=pl.ANY)
    return pl.pallas_call(
        functools.partial(keep_kernel, parts),
        out_shape=(whole, whole, line, line),
        in_specs=[near] * 4,
        out_specs=(anywhere,) * 4,
        scratch_shapes=[
            [pltpu.VMEM((columns,), jnp.float32)] * 2,
            pltpu.SemaphoreType.DMA((2,)),
            pltpu.SemaphoreType.DMA((2,)),
        ],
        compiler_params=pltpu.CompilerParams(vmem_limit_bytes=2**20),
        cost_estimate=pl.CostEstimate(flops=100 * gate.size, bytes_accessed=4 * gate.size, transcendentals=0),
        name="keep",
    )(gate, up, factor_gate, factor_up)


def close_kernel(n, ahead_ref, back_ref, in_ref, out_ref, sem):
    place = ring_place(lax.axis_index("rows"), n)
    size = ahead_ref.shape[0]
    rows = out_ref.shape[0] // n
    copies = []
    for way, (src, turn) in enumerate(((ahead_ref, 1), (back_ref, n - 1))):
        first = ring_row((place + turn) % n, n) * rows + way * (rows // 2)
        copies.append(pltpu.make_async_copy(src, out_ref.at[pl.ds(pl.multiple_of(first, 16), size)], sem.at[way]))
        copies[-1].start()
    for copy in copies:
        copy.wait()


def close(n, ahead, back, gate):
    near = pl.BlockSpec(memory_space=pltpu.VMEM)
    anywhere = pl.BlockSpec(memory_space=pl.ANY)
    ahead, back = (pltpu.with_memory_space_constraint(t, pltpu.VMEM) for t in (ahead, back))
    return pl.pallas_call(
        functools.partial(close_kernel, n),
        out_shape=jax.ShapeDtypeStruct(gate.shape, gate.dtype),
        in_specs=[near, near, anywhere],
        out_specs=anywhere,
        scratch_shapes=[pltpu.SemaphoreType.DMA((2,))],
        input_output_aliases={2: 0},
        compiler_params=pltpu.CompilerParams(vmem_limit_bytes=2**20),
        name="close",
    )(ahead, back, gate)


def local(n, w_gate, avg_gate, w_up, avg_up, norm_gain):
    gate, up, factor_gate, factor_up, ahead, back = serve(w_gate, avg_gate, w_up, avg_up, norm_gain, n)
    ring = [ring_row(p, n) for p in range(n)]
    pairs = [(ring[p], ring[(p + 1) % n]) for p in range(n)]
    ahead = lax.ppermute(ahead, "rows", pairs)
    back = lax.ppermute(back, "rows", [(b, a) for a, b in pairs])
    gate, up, factor_gate, factor_up = keep(gate, up, factor_gate, factor_up)
    return (close(n, ahead, back, gate), up, factor_gate, factor_up)


def solution(mesh):
    placed = (P("rows", "width"),) * 4 + (P("rows"),)
    return jax.shard_map(
        functools.partial(local, mesh.shape["rows"]),
        mesh=mesh,
        in_specs=placed,
        out_specs=(P(None, "width"), P(None, "width"), P("width"), P("width")),
        check_vma=False,
    )
```

```python
import functools

import jax
import jax.numpy as jnp
from jax import lax
from jax.experimental import pallas as pl
from jax.experimental.pallas import tpu as pltpu
from jax.sharding import PartitionSpec as P

keep_rate = 0.7
MESH = pl.DeviceIdType.MESH
TAIL = 112
SPLIT = 16
EARLY = 16
FIRST = 16
KEEP = 8
VMEM_LIMIT = 36 * 2**20


def ring_place(r, n):
    if n % 2:
        return r
    x, z = r % 2, r // 2
    return z + x * (n - 1 - 2 * z)


def ring_row(p, n):
    if n % 2:
        return p
    half = n // 2
    x, k = p // half, p % half
    return 2 * (k + x * (half - 1 - 2 * k)) + x


def serve_kernel(
    n, size, gain_ref, wg_ref, ag_ref, wu_ref, au_ref,
    go_ref, uo_ref, fg_ref, fu_ref, gt_ref, ut_ref,
    w_in, fresh, early, gains, part, got,
    in_sem, max_send, max_recv, early_send, early_recv, send_sem, recv_sem, tail_sem,
):
    me = lax.axis_index("rows")
    barrier = pltpu.get_barrier_semaphore()
    for d in range(1, n):
        pl.semaphore_signal(barrier, inc=1, device_id={"rows": (me + d) % n}, device_id_type=MESH)

    place = ring_place(me, n)
    nxt = ring_row((place + 1) % n, n)
    prv = ring_row((place + n - 1) % n, n)
    rows, columns = wg_ref.shape
    half = rows // 2
    outs, to = (go_ref, uo_ref), (nxt, prv)
    ins = ((wg_ref, ag_ref), (wu_ref, au_ref))

    spans = [(0, way * half, FIRST) for way in range(2)]
    spans += [(0, way * half + FIRST, half - FIRST) for way in range(2)]
    spans += [(1, way * half, half) for way in range(2)]
    for s, (k, first, count) in enumerate(spans):
        at = pl.ds(first, count)
        for j, dst in enumerate((w_in, fresh)):
            load = pltpu.make_async_copy(ins[k][j].at[at], dst.at[k, at], in_sem.at[s])
            load.start()

    for first in range(0, rows, 128):
        count = min(128, rows - first)
        line = gain_ref[first : first + count].reshape(1, count)
        gains[first : first + count, :] = jnp.broadcast_to(line, (128, count)).T

    def blend(s, top):
        k, first, count = spans[s]
        both = fresh.at[:, pl.ds(0, count)]
        pltpu.make_async_copy(both, both, in_sem.at[s]).wait()

        def body(i, top):
            at = pl.ds(pl.multiple_of(first + i * 8, 8), 8)
            gain = jnp.tile(gains[at, :], (1, columns // 128))
            value = (keep_rate * fresh[k, at, :] + (1.0 - keep_rate) * w_in[k, at, :]) * gain
            fresh[k, at, :] = value
            return jnp.maximum(top, jnp.abs(value))

        return lax.fori_loop(0, count // 8, body, top)

    cuts = ((0, SPLIT),)

    def ahead(way, b):
        first, end = cuts[b]
        return pltpu.make_async_remote_copy(
            src_ref=fresh.at[0, pl.ds(way * half + first, end - first)],
            dst_ref=early.at[way, pl.ds(first, end - first)],
            send_sem=early_send.at[way],
            recv_sem=early_recv.at[way],
            device_id={"rows": to[way]},
            device_id_type=MESH,
        )

    def spread(k, top):
        part[k] = jnp.max(top, axis=0, keepdims=True)
        for d in range(1, n):
            pltpu.make_async_remote_copy(
                src_ref=part.at[k],
                dst_ref=got.at[k, d - 1],
                send_sem=max_send.at[k],
                recv_sem=max_recv.at[k],
                device_id={"rows": (me + d) % n},
                device_id_type=MESH,
            ).start()

    def drained(ref, sem):
        pltpu.make_async_copy(ref, ref, sem).wait()

    def gather(k, out):
        drained(got.at[k], max_recv.at[k])
        factor = part[k]
        for d in range(n - 1):
            factor = jnp.maximum(factor, got[k, d])
        out[...] = factor
        return 1.0 / factor

    top = jnp.zeros((8, columns), jnp.float32)
    top = blend(0, top)
    top = blend(1, top)
    pl.semaphore_wait(barrier, n - 1)
    for way in range(2):
        ahead(way, 0).start()
    top = blend(2, top)
    top = blend(3, top)
    spread(0, top)
    top = jnp.zeros((8, columns), jnp.float32)
    top = blend(4, top)
    top = blend(5, top)
    spread(1, top)

    pieces = [(k, first, count) for k in range(2) for first, count in ((0, size), (size, half - size))]
    chunks = len(pieces)

    def block(turn):
        return ring_row((place + turn) % n, n) * rows

    def turn_out(way, step):
        return (n - step) if way == 0 else step

    def turn_in(way, step):
        return (n - step - 1) if way == 0 else (step + 1)

    def moved(way, step, q, turn, skip=0):
        k, first, count = pieces[q]
        first += way * half + skip
        at = outs[k].at[pl.ds(pl.multiple_of(block(turn) + first, 16), count - skip)]
        return pltpu.make_async_remote_copy(
            src_ref=at,
            dst_ref=at,
            send_sem=send_sem.at[way],
            recv_sem=recv_sem.at[way, step, q],
            device_id={"rows": to[way]},
            device_id_type=MESH,
        )

    def send(way, step, q, skip=0):
        return moved(way, step, q, turn_out(way, step), skip)

    def landed(way, step, q, skip=0):
        moved(way, step, q, turn_in(way, step), skip).wait_recv()

    def narrow(k, scale, load, first, count, base):
        by = jnp.broadcast_to(scale, (16, columns))

        @pl.loop(0, count // 16)
        def _(i):
            to_at = pl.ds(pl.multiple_of(base + i * 16, 16), 16)
            outs[k][to_at, :] = (load(pl.ds(pl.multiple_of(first + i * 16, 16), 16)) * by).astype(jnp.bfloat16)

    skips = [EARLY] + [0] * (chunks - 1)
    pending = []
    scales = []
    for q, (k, first, count) in enumerate(pieces):
        if k == len(scales):
            scales.append(gather(k, (fg_ref, fu_ref)[k]))
        for way in range(2):
            at = way * half + first + skips[q]
            narrow(k, scales[k], lambda at: fresh[k, at, :], at, count - skips[q], block(0) + at)
            pending.append(send(way, 0, q, skips[q]))
            if len(pending) > 1:
                pending.pop(0).start()
    pending.pop(0).start()
    for way in range(2):
        drained(early.at[way], early_recv.at[way])
        narrow(0, scales[0], lambda at: early[way, at, :], 0, EARLY, block(turn_in(way, 0)) + way * half)
    for way in range(2):
        narrow(0, scales[0], lambda at: fresh[0, at, :], way * half, EARLY, block(0) + way * half)

    for q in range(chunks):
        for way in range(2):
            landed(way, 0, q, skips[q])
            send(way, 1, q).start()

    @pl.loop(2, n - 2)
    def _(step):
        for q in range(chunks):
            for way in range(2):
                landed(way, step - 1, q)
                send(way, step, q).start()

    last = n - 2
    for way in range(2):
        landed(way, last - 1, 0)
    tails = []
    for way, ref in enumerate((gt_ref, ut_ref)):
        at = pl.ds(pl.multiple_of(block(turn_out(way, last)) + way * half, 16), size)
        copy = pltpu.make_async_copy(go_ref.at[at], ref, tail_sem.at[way])
        copy.start()
        tails.append(copy)
    for q in range(1, chunks):
        for way in range(2):
            landed(way, last - 1, q)
            send(way, last, q).start()
    for copy in tails:
        copy.wait()

    for q in range(1, chunks):
        for way in range(2):
            landed(way, last, q)
    for way in range(2):
        drained(early.at[way], early_send.at[way])
        drained(got.at[way], max_send.at[way])
        sent = go_ref.at[pl.ds(0, (n - 1) * rows - EARLY - size)]
        drained(sent, send_sem.at[way])


def serve(w_gate, avg_gate, w_up, avg_up, norm_gain, n):
    rows, columns = w_gate.shape
    half = rows // 2
    size = min(TAIL, half // 32 * 16 + 16)
    whole = pltpu.VMEM((n * rows, columns), jnp.bfloat16)
    tail = pltpu.HBM((size, columns), jnp.bfloat16)
    line = pltpu.VMEM((1, columns), jnp.float32)
    anywhere = pl.BlockSpec(memory_space=pl.ANY)
    near = pl.BlockSpec(memory_space=pltpu.VMEM)
    return pl.pallas_call(
        functools.partial(serve_kernel, n, size),
        out_shape=(whole, whole, line, line, tail, tail),
        in_specs=[near] + [anywhere] * 4,
        out_specs=(near, near, near, near, anywhere, anywhere),
        scratch_shapes=[
            pltpu.VMEM((2, rows, columns), jnp.float32),
            pltpu.VMEM((2, rows, columns), jnp.float32),
            pltpu.VMEM((2, EARLY, columns), jnp.float32),
            pltpu.VMEM((rows, 128), jnp.float32),
            pltpu.VMEM((2, 1, columns), jnp.float32),
            pltpu.VMEM((2, n - 1, 1, columns), jnp.float32),
            pltpu.SemaphoreType.DMA((6,)),
            pltpu.SemaphoreType.DMA((2,)),
            pltpu.SemaphoreType.DMA((2,)),
            pltpu.SemaphoreType.DMA((2,)),
            pltpu.SemaphoreType.DMA((2,)),
            pltpu.SemaphoreType.DMA((2,)),
            pltpu.SemaphoreType.DMA((2, n - 1, 4)),
            pltpu.SemaphoreType.DMA((2,)),
        ],
        compiler_params=pltpu.CompilerParams(
            collective_id=0, has_side_effects=True, vmem_limit_bytes=VMEM_LIMIT
        ),
        name="serve",
    )(norm_gain, w_gate, avg_gate, w_up, avg_up)


def keep_kernel(parts, gate_ref, up_ref, fg_ref, fu_ref, go_ref, uo_ref, fgo_ref, fuo_ref, lines, sem, line_sem):
    size = gate_ref.shape[0] // parts
    for c in range(parts):
        at = pl.ds(c * size, size)
        for k, (src, dst) in enumerate(((gate_ref, go_ref), (up_ref, uo_ref))):
            pltpu.make_async_copy(src.at[at], dst.at[at], sem.at[k]).start()
    for k, (src, dst) in enumerate(((fg_ref, fgo_ref), (fu_ref, fuo_ref))):
        lines[k][...] = src[0]
        pltpu.make_async_copy(lines[k], dst, line_sem.at[k]).start()
    for k, (ref, out, line) in enumerate(((gate_ref, go_ref, fgo_ref), (up_ref, uo_ref, fuo_ref))):
        pltpu.make_async_copy(ref, out, sem.at[k]).wait()
        pltpu.make_async_copy(lines[k], line, line_sem.at[k]).wait()


def keep(gate, up, factor_gate, factor_up):
    parts = KEEP
    columns = gate.shape[1]
    whole = jax.ShapeDtypeStruct(gate.shape, gate.dtype)
    line = jax.ShapeDtypeStruct((columns,), factor_gate.dtype)
    near = pl.BlockSpec(memory_space=pltpu.VMEM)
    anywhere = pl.BlockSpec(memory_space=pl.ANY)
    return pl.pallas_call(
        functools.partial(keep_kernel, parts),
        out_shape=(whole, whole, line, line),
        in_specs=[near] * 4,
        out_specs=(anywhere,) * 4,
        scratch_shapes=[
            [pltpu.VMEM((columns,), jnp.float32)] * 2,
            pltpu.SemaphoreType.DMA((2,)),
            pltpu.SemaphoreType.DMA((2,)),
        ],
        compiler_params=pltpu.CompilerParams(vmem_limit_bytes=2**20),
        cost_estimate=pl.CostEstimate(flops=100 * gate.size, bytes_accessed=4 * gate.size, transcendentals=0),
        name="keep",
    )(gate, up, factor_gate, factor_up)


def close_kernel(n, ahead_ref, back_ref, in_ref, out_ref, sem):
    place = ring_place(lax.axis_index("rows"), n)
    size = ahead_ref.shape[0]
    rows = out_ref.shape[0] // n
    copies = []
    for way, (src, turn) in enumerate(((ahead_ref, 1), (back_ref, n - 1))):
        first = ring_row((place + turn) % n, n) * rows + way * (rows // 2)
        copies.append(pltpu.make_async_copy(src, out_ref.at[pl.ds(pl.multiple_of(first, 16), size)], sem.at[way]))
        copies[-1].start()
    for copy in copies:
        copy.wait()


def close(n, ahead, back, gate):
    near = pl.BlockSpec(memory_space=pltpu.VMEM)
    anywhere = pl.BlockSpec(memory_space=pl.ANY)
    ahead, back = (pltpu.with_memory_space_constraint(t, pltpu.VMEM) for t in (ahead, back))
    return pl.pallas_call(
        functools.partial(close_kernel, n),
        out_shape=jax.ShapeDtypeStruct(gate.shape, gate.dtype),
        in_specs=[near, near, anywhere],
        out_specs=anywhere,
        scratch_shapes=[pltpu.SemaphoreType.DMA((2,))],
        input_output_aliases={2: 0},
        compiler_params=pltpu.CompilerParams(vmem_limit_bytes=2**20),
        name="close",
    )(ahead, back, gate)


def local(n, w_gate, avg_gate, w_up, avg_up, norm_gain):
    gate, up, factor_gate, factor_up, ahead, back = serve(w_gate, avg_gate, w_up, avg_up, norm_gain, n)
    ring = [ring_row(p, n) for p in range(n)]
    pairs = [(ring[p], ring[(p + 1) % n]) for p in range(n)]
    ahead = lax.ppermute(ahead, "rows", pairs)
    back = lax.ppermute(back, "rows", [(b, a) for a, b in pairs])
    gate, up, factor_gate, factor_up = keep(gate, up, factor_gate, factor_up)
    return (close(n, ahead, back, gate), up, factor_gate, factor_up)


def solution(mesh):
    placed = (P("rows", "width"),) * 4 + (P("rows"),)
    return jax.shard_map(
        functools.partial(local, mesh.shape["rows"]),
        mesh=mesh,
        in_specs=placed,
        out_specs=(P(None, "width"), P(None, "width"), P("width"), P("width")),
        check_vma=False,
    )
```

```python
import functools

import jax
import jax.numpy as jnp
from jax import lax
from jax.experimental import pallas as pl
from jax.experimental.pallas import tpu as pltpu
from jax.sharding import PartitionSpec as P

keep_rate = 0.7
MESH = pl.DeviceIdType.MESH
TAIL = 112
SPLIT = 16
EARLY = 16
FIRST = 16
KEEP = 16
VMEM_LIMIT = 36 * 2**20


def ring_place(r, n):
    if n % 2:
        return r
    x, z = r % 2, r // 2
    return z + x * (n - 1 - 2 * z)


def ring_row(p, n):
    if n % 2:
        return p
    half = n // 2
    x, k = p // half, p % half
    return 2 * (k + x * (half - 1 - 2 * k)) + x


def serve_kernel(
    n, size, gain_ref, wg_ref, ag_ref, wu_ref, au_ref,
    go_ref, uo_ref, fg_ref, fu_ref, gt_ref, ut_ref,
    w_in, fresh, early, gains, part, got,
    in_sem, max_send, max_recv, early_send, early_recv, send_sem, recv_sem, tail_sem,
):
    me = lax.axis_index("rows")
    barrier = pltpu.get_barrier_semaphore()
    for d in range(1, n):
        pl.semaphore_signal(barrier, inc=1, device_id={"rows": (me + d) % n}, device_id_type=MESH)

    place = ring_place(me, n)
    nxt = ring_row((place + 1) % n, n)
    prv = ring_row((place + n - 1) % n, n)
    rows, columns = wg_ref.shape
    half = rows // 2
    outs, to = (go_ref, uo_ref), (nxt, prv)
    ins = ((wg_ref, ag_ref), (wu_ref, au_ref))

    spans = [(0, way * half, FIRST) for way in range(2)]
    spans += [(0, way * half + FIRST, half - FIRST) for way in range(2)]
    spans += [(1, way * half, half) for way in range(2)]
    for s, (k, first, count) in enumerate(spans):
        at = pl.ds(first, count)
        for j, dst in enumerate((w_in, fresh)):
            load = pltpu.make_async_copy(ins[k][j].at[at], dst.at[k, at], in_sem.at[s])
            load.start()

    for first in range(0, rows, 128):
        count = min(128, rows - first)
        line = gain_ref[first : first + count].reshape(1, count)
        gains[first : first + count, :] = jnp.broadcast_to(line, (128, count)).T

    def blend(s, top):
        k, first, count = spans[s]
        both = fresh.at[:, pl.ds(0, count)]
        pltpu.make_async_copy(both, both, in_sem.at[s]).wait()

        def body(i, top):
            at = pl.ds(pl.multiple_of(first + i * 8, 8), 8)
            gain = jnp.tile(gains[at, :], (1, columns // 128))
            value = (keep_rate * fresh[k, at, :] + (1.0 - keep_rate) * w_in[k, at, :]) * gain
            fresh[k, at, :] = value
            return jnp.maximum(top, jnp.abs(value))

        return lax.fori_loop(0, count // 8, body, top)

    cuts = ((0, SPLIT),)

    def ahead(way, b):
        first, end = cuts[b]
        return pltpu.make_async_remote_copy(
            src_ref=fresh.at[0, pl.ds(way * half + first, end - first)],
            dst_ref=early.at[way, pl.ds(first, end - first)],
            send_sem=early_send.at[way],
            recv_sem=early_recv.at[way],
            device_id={"rows": to[way]},
            device_id_type=MESH,
        )

    def spread(k, top):
        part[k] = jnp.max(top, axis=0, keepdims=True)
        for d in range(1, n):
            pltpu.make_async_remote_copy(
                src_ref=part.at[k],
                dst_ref=got.at[k, d - 1],
                send_sem=max_send.at[k],
                recv_sem=max_recv.at[k],
                device_id={"rows": (me + d) % n},
                device_id_type=MESH,
            ).start()

    def drained(ref, sem):
        pltpu.make_async_copy(ref, ref, sem).wait()

    def gather(k, out):
        drained(got.at[k], max_recv.at[k])
        factor = part[k]
        for d in range(n - 1):
            factor = jnp.maximum(factor, got[k, d])
        out[...] = factor
        return 1.0 / factor

    top = jnp.zeros((8, columns), jnp.float32)
    top = blend(0, top)
    top = blend(1, top)
    pl.semaphore_wait(barrier, n - 1)
    for way in range(2):
        ahead(way, 0).start()
    top = blend(2, top)
    top = blend(3, top)
    spread(0, top)
    top = jnp.zeros((8, columns), jnp.float32)
    top = blend(4, top)
    top = blend(5, top)
    spread(1, top)

    pieces = [(k, first, count) for k in range(2) for first, count in ((0, size), (size, half - size))]
    chunks = len(pieces)

    def block(turn):
        return ring_row((place + turn) % n, n) * rows

    def turn_out(way, step):
        return (n - step) if way == 0 else step

    def turn_in(way, step):
        return (n - step - 1) if way == 0 else (step + 1)

    def moved(way, step, q, turn, skip=0):
        k, first, count = pieces[q]
        first += way * half + skip
        at = outs[k].at[pl.ds(pl.multiple_of(block(turn) + first, 16), count - skip)]
        return pltpu.make_async_remote_copy(
            src_ref=at,
            dst_ref=at,
            send_sem=send_sem.at[way],
            recv_sem=recv_sem.at[way, step, q],
            device_id={"rows": to[way]},
            device_id_type=MESH,
        )

    def send(way, step, q, skip=0):
        return moved(way, step, q, turn_out(way, step), skip)

    def landed(way, step, q, skip=0):
        moved(way, step, q, turn_in(way, step), skip).wait_recv()

    def narrow(k, scale, load, first, count, base):
        by = jnp.broadcast_to(scale, (16, columns))

        @pl.loop(0, count // 16)
        def _(i):
            to_at = pl.ds(pl.multiple_of(base + i * 16, 16), 16)
            outs[k][to_at, :] = (load(pl.ds(pl.multiple_of(first + i * 16, 16), 16)) * by).astype(jnp.bfloat16)

    skips = [EARLY] + [0] * (chunks - 1)
    pending = []
    scales = []
    for q, (k, first, count) in enumerate(pieces):
        if k == len(scales):
            scales.append(gather(k, (fg_ref, fu_ref)[k]))
        for way in range(2):
            at = way * half + first + skips[q]
            narrow(k, scales[k], lambda at: fresh[k, at, :], at, count - skips[q], block(0) + at)
            pending.append(send(way, 0, q, skips[q]))
            if len(pending) > 1:
                pending.pop(0).start()
    pending.pop(0).start()
    for way in range(2):
        drained(early.at[way], early_recv.at[way])
        narrow(0, scales[0], lambda at: early[way, at, :], 0, EARLY, block(turn_in(way, 0)) + way * half)
    for way in range(2):
        narrow(0, scales[0], lambda at: fresh[0, at, :], way * half, EARLY, block(0) + way * half)

    for q in range(chunks):
        for way in range(2):
            landed(way, 0, q, skips[q])
            send(way, 1, q).start()

    @pl.loop(2, n - 2)
    def _(step):
        for q in range(chunks):
            for way in range(2):
                landed(way, step - 1, q)
                send(way, step, q).start()

    last = n - 2
    for way in range(2):
        landed(way, last - 1, 0)
    tails = []
    for way, ref in enumerate((gt_ref, ut_ref)):
        at = pl.ds(pl.multiple_of(block(turn_out(way, last)) + way * half, 16), size)
        copy = pltpu.make_async_copy(go_ref.at[at], ref, tail_sem.at[way])
        copy.start()
        tails.append(copy)
    for q in range(1, chunks):
        for way in range(2):
            landed(way, last - 1, q)
            send(way, last, q).start()
    for copy in tails:
        copy.wait()

    for q in range(1, chunks):
        for way in range(2):
            landed(way, last, q)
    for way in range(2):
        drained(early.at[way], early_send.at[way])
        drained(got.at[way], max_send.at[way])
        sent = go_ref.at[pl.ds(0, (n - 1) * rows - EARLY - size)]
        drained(sent, send_sem.at[way])


def serve(w_gate, avg_gate, w_up, avg_up, norm_gain, n):
    rows, columns = w_gate.shape
    half = rows // 2
    size = min(TAIL, half // 32 * 16 + 16)
    whole = pltpu.VMEM((n * rows, columns), jnp.bfloat16)
    tail = pltpu.HBM((size, columns), jnp.bfloat16)
    line = pltpu.VMEM((1, columns), jnp.float32)
    anywhere = pl.BlockSpec(memory_space=pl.ANY)
    near = pl.BlockSpec(memory_space=pltpu.VMEM)
    return pl.pallas_call(
        functools.partial(serve_kernel, n, size),
        out_shape=(whole, whole, line, line, tail, tail),
        in_specs=[near] + [anywhere] * 4,
        out_specs=(near, near, near, near, anywhere, anywhere),
        scratch_shapes=[
            pltpu.VMEM((2, rows, columns), jnp.float32),
            pltpu.VMEM((2, rows, columns), jnp.float32),
            pltpu.VMEM((2, EARLY, columns), jnp.float32),
            pltpu.VMEM((rows, 128), jnp.float32),
            pltpu.VMEM((2, 1, columns), jnp.float32),
            pltpu.VMEM((2, n - 1, 1, columns), jnp.float32),
            pltpu.SemaphoreType.DMA((6,)),
            pltpu.SemaphoreType.DMA((2,)),
            pltpu.SemaphoreType.DMA((2,)),
            pltpu.SemaphoreType.DMA((2,)),
            pltpu.SemaphoreType.DMA((2,)),
            pltpu.SemaphoreType.DMA((2,)),
            pltpu.SemaphoreType.DMA((2, n - 1, 4)),
            pltpu.SemaphoreType.DMA((2,)),
        ],
        compiler_params=pltpu.CompilerParams(
            collective_id=0, has_side_effects=True, vmem_limit_bytes=VMEM_LIMIT
        ),
        name="serve",
    )(norm_gain, w_gate, avg_gate, w_up, avg_up)


def keep_kernel(parts, gate_ref, up_ref, fg_ref, fu_ref, go_ref, uo_ref, fgo_ref, fuo_ref, lines, sem, line_sem):
    size = gate_ref.shape[0] // parts
    for c in range(parts):
        at = pl.ds(c * size, size)
        for k, (src, dst) in enumerate(((gate_ref, go_ref), (up_ref, uo_ref))):
            pltpu.make_async_copy(src.at[at], dst.at[at], sem.at[k]).start()
    for k, (src, dst) in enumerate(((fg_ref, fgo_ref), (fu_ref, fuo_ref))):
        lines[k][...] = src[0]
        pltpu.make_async_copy(lines[k], dst, line_sem.at[k]).start()
    for k, (ref, out, line) in enumerate(((gate_ref, go_ref, fgo_ref), (up_ref, uo_ref, fuo_ref))):
        pltpu.make_async_copy(ref, out, sem.at[k]).wait()
        pltpu.make_async_copy(lines[k], line, line_sem.at[k]).wait()


def keep(gate, up, factor_gate, factor_up):
    parts = KEEP
    columns = gate.shape[1]
    whole = jax.ShapeDtypeStruct(gate.shape, gate.dtype)
    line = jax.ShapeDtypeStruct((columns,), factor_gate.dtype)
    near = pl.BlockSpec(memory_space=pltpu.VMEM)
    anywhere = pl.BlockSpec(memory_space=pl.ANY)
    return pl.pallas_call(
        functools.partial(keep_kernel, parts),
        out_shape=(whole, whole, line, line),
        in_specs=[near] * 4,
        out_specs=(anywhere,) * 4,
        scratch_shapes=[
            [pltpu.VMEM((columns,), jnp.float32)] * 2,
            pltpu.SemaphoreType.DMA((2,)),
            pltpu.SemaphoreType.DMA((2,)),
        ],
        compiler_params=pltpu.CompilerParams(vmem_limit_bytes=2**20),
        cost_estimate=pl.CostEstimate(flops=100 * gate.size, bytes_accessed=4 * gate.size, transcendentals=0),
        name="keep",
    )(gate, up, factor_gate, factor_up)


def close_kernel(n, way, tail_ref, in_ref, out_ref, sem):
    place = ring_place(lax.axis_index("rows"), n)
    rows = out_ref.shape[0] // n
    first = ring_row((place + (1, n - 1)[way]) % n, n) * rows + way * (rows // 2)
    at = pl.ds(pl.multiple_of(first, 16), tail_ref.shape[0])
    copy = pltpu.make_async_copy(tail_ref, out_ref.at[at], sem)
    copy.start()
    copy.wait()


def close(n, way, tail, gate):
    near = pl.BlockSpec(memory_space=pltpu.VMEM)
    anywhere = pl.BlockSpec(memory_space=pl.ANY)
    return pl.pallas_call(
        functools.partial(close_kernel, n, way),
        out_shape=jax.ShapeDtypeStruct(gate.shape, gate.dtype),
        in_specs=[near, anywhere],
        out_specs=anywhere,
        scratch_shapes=[pltpu.SemaphoreType.DMA],
        input_output_aliases={1: 0},
        compiler_params=pltpu.CompilerParams(vmem_limit_bytes=2**20),
        name="close",
    )(pltpu.with_memory_space_constraint(tail, pltpu.VMEM), gate)


def local(n, w_gate, avg_gate, w_up, avg_up, norm_gain):
    gate, up, factor_gate, factor_up, ahead, back = serve(w_gate, avg_gate, w_up, avg_up, norm_gain, n)
    ring = [ring_row(p, n) for p in range(n)]
    pairs = [(ring[p], ring[(p + 1) % n]) for p in range(n)]
    ahead = lax.ppermute(ahead, "rows", pairs)
    back = lax.ppermute(back, "rows", [(b, a) for a, b in pairs])
    gate, up, factor_gate, factor_up = keep(gate, up, factor_gate, factor_up)
    return (close(n, 1, back, close(n, 0, ahead, gate)), up, factor_gate, factor_up)


def solution(mesh):
    placed = (P("rows", "width"),) * 4 + (P("rows"),)
    return jax.shard_map(
        functools.partial(local, mesh.shape["rows"]),
        mesh=mesh,
        in_specs=placed,
        out_specs=(P(None, "width"), P(None, "width"), P("width"), P("width")),
        check_vma=False,
    )
```

```python
import functools

import jax
import jax.numpy as jnp
from jax import lax
from jax.experimental import pallas as pl
from jax.experimental.pallas import tpu as pltpu
from jax.sharding import PartitionSpec as P

keep_rate = 0.7
MESH = pl.DeviceIdType.MESH
TAIL = 112
SPLIT = 16
EARLY = 16
FIRST = 16
KEEP = 16
VMEM_LIMIT = 36 * 2**20


def ring_place(r, n):
    if n % 2:
        return r
    x, z = r % 2, r // 2
    return z + x * (n - 1 - 2 * z)


def ring_row(p, n):
    if n % 2:
        return p
    half = n // 2
    x, k = p // half, p % half
    return 2 * (k + x * (half - 1 - 2 * k)) + x


def serve_kernel(
    n, size, gain_ref, wg_ref, ag_ref, wu_ref, au_ref,
    go_ref, uo_ref, fg_ref, fu_ref, gt_ref, ut_ref,
    w_in, fresh, early, gains, part, got,
    in_sem, max_send, max_recv, early_send, early_recv, send_sem, recv_sem,
):
    me = lax.axis_index("rows")
    barrier = pltpu.get_barrier_semaphore()
    for d in range(1, n):
        pl.semaphore_signal(barrier, inc=1, device_id={"rows": (me + d) % n}, device_id_type=MESH)

    place = ring_place(me, n)
    nxt = ring_row((place + 1) % n, n)
    prv = ring_row((place + n - 1) % n, n)
    rows, columns = wg_ref.shape
    half = rows // 2
    outs, to = (go_ref, uo_ref), (nxt, prv)
    ins = ((wg_ref, ag_ref), (wu_ref, au_ref))

    spans = [(0, way * half, FIRST) for way in range(2)]
    spans += [(0, way * half + FIRST, half - FIRST) for way in range(2)]
    spans += [(1, way * half, half) for way in range(2)]
    for s, (k, first, count) in enumerate(spans):
        at = pl.ds(first, count)
        for j, dst in enumerate((w_in, fresh)):
            load = pltpu.make_async_copy(ins[k][j].at[at], dst.at[k, at], in_sem.at[s])
            load.start()

    for first in range(0, rows, 128):
        count = min(128, rows - first)
        line = gain_ref[first : first + count].reshape(1, count)
        gains[first : first + count, :] = jnp.broadcast_to(line, (128, count)).T

    def blend(s, top):
        k, first, count = spans[s]
        both = fresh.at[:, pl.ds(0, count)]
        pltpu.make_async_copy(both, both, in_sem.at[s]).wait()

        def body(i, top):
            at = pl.ds(pl.multiple_of(first + i * 8, 8), 8)
            gain = jnp.tile(gains[at, :], (1, columns // 128))
            value = (keep_rate * fresh[k, at, :] + (1.0 - keep_rate) * w_in[k, at, :]) * gain
            fresh[k, at, :] = value
            return jnp.maximum(top, jnp.abs(value))

        return lax.fori_loop(0, count // 8, body, top)

    cuts = ((0, SPLIT),)

    def ahead(way, b):
        first, end = cuts[b]
        return pltpu.make_async_remote_copy(
            src_ref=fresh.at[0, pl.ds(way * half + first, end - first)],
            dst_ref=early.at[way, pl.ds(first, end - first)],
            send_sem=early_send.at[way],
            recv_sem=early_recv.at[way],
            device_id={"rows": to[way]},
            device_id_type=MESH,
        )

    def spread(k, top):
        part[k] = jnp.max(top, axis=0, keepdims=True)
        for d in range(1, n):
            pltpu.make_async_remote_copy(
                src_ref=part.at[k],
                dst_ref=got.at[k, d - 1],
                send_sem=max_send.at[k],
                recv_sem=max_recv.at[k],
                device_id={"rows": (me + d) % n},
                device_id_type=MESH,
            ).start()

    def drained(ref, sem):
        pltpu.make_async_copy(ref, ref, sem).wait()

    def gather(k, out):
        drained(got.at[k], max_recv.at[k])
        factor = part[k]
        for d in range(n - 1):
            factor = jnp.maximum(factor, got[k, d])
        out[...] = factor
        return 1.0 / factor

    top = jnp.zeros((8, columns), jnp.float32)
    top = blend(0, top)
    top = blend(1, top)
    pl.semaphore_wait(barrier, n - 1)
    for way in range(2):
        ahead(way, 0).start()
    top = blend(2, top)
    top = blend(3, top)
    spread(0, top)
    top = jnp.zeros((8, columns), jnp.float32)
    top = blend(4, top)
    top = blend(5, top)
    spread(1, top)

    pieces = [(k, first, count) for k in range(2) for first, count in ((0, size), (size, half - size))]
    chunks = len(pieces)

    def block(turn):
        return ring_row((place + turn) % n, n) * rows

    def turn_out(way, step):
        return (n - step) if way == 0 else step

    def turn_in(way, step):
        return (n - step - 1) if way == 0 else (step + 1)

    def moved(way, step, q, turn, skip=0):
        k, first, count = pieces[q]
        first += way * half + skip
        at = outs[k].at[pl.ds(pl.multiple_of(block(turn) + first, 16), count - skip)]
        return pltpu.make_async_remote_copy(
            src_ref=at,
            dst_ref=at,
            send_sem=send_sem.at[way],
            recv_sem=recv_sem.at[way, step, q],
            device_id={"rows": to[way]},
            device_id_type=MESH,
        )

    def send(way, step, q, skip=0):
        return moved(way, step, q, turn_out(way, step), skip)

    def landed(way, step, q, skip=0):
        moved(way, step, q, turn_in(way, step), skip).wait_recv()

    def narrow(k, scale, load, first, count, base):
        by = jnp.broadcast_to(scale, (16, columns))

        @pl.loop(0, count // 16)
        def _(i):
            to_at = pl.ds(pl.multiple_of(base + i * 16, 16), 16)
            outs[k][to_at, :] = (load(pl.ds(pl.multiple_of(first + i * 16, 16), 16)) * by).astype(jnp.bfloat16)

    skips = [EARLY] + [0] * (chunks - 1)
    pending = []
    scales = []
    for q, (k, first, count) in enumerate(pieces):
        if k == len(scales):
            scales.append(gather(k, (fg_ref, fu_ref)[k]))
        for way in range(2):
            at = way * half + first + skips[q]
            narrow(k, scales[k], lambda at: fresh[k, at, :], at, count - skips[q], block(0) + at)
            pending.append(send(way, 0, q, skips[q]))
            if len(pending) > 1:
                pending.pop(0).start()
    pending.pop(0).start()
    for way in range(2):
        drained(early.at[way], early_recv.at[way])
        narrow(0, scales[0], lambda at: early[way, at, :], 0, EARLY, block(turn_in(way, 0)) + way * half)
    for way in range(2):
        narrow(0, scales[0], lambda at: fresh[0, at, :], way * half, EARLY, block(0) + way * half)

    for q in range(chunks):
        for way in range(2):
            landed(way, 0, q, skips[q])
            send(way, 1, q).start()

    @pl.loop(2, n - 2)
    def _(step):
        for q in range(chunks):
            for way in range(2):
                landed(way, step - 1, q)
                send(way, step, q).start()

    last = n - 2
    for way in range(2):
        landed(way, last - 1, 0)
    for way, ref in enumerate((gt_ref, ut_ref)):
        base = block(turn_out(way, last)) + way * half

        @pl.loop(0, size // 16)
        def _(i):
            at = pl.ds(pl.multiple_of(base + i * 16, 16), 16)
            ref[pl.ds(pl.multiple_of(i * 16, 16), 16), :] = go_ref[at, :]

    for q in range(1, chunks):
        for way in range(2):
            landed(way, last - 1, q)
            send(way, last, q).start()

    for q in range(1, chunks):
        for way in range(2):
            landed(way, last, q)
    for way in range(2):
        drained(early.at[way], early_send.at[way])
        drained(got.at[way], max_send.at[way])
        sent = go_ref.at[pl.ds(0, (n - 1) * rows - EARLY - size)]
        drained(sent, send_sem.at[way])


def serve(w_gate, avg_gate, w_up, avg_up, norm_gain, n):
    rows, columns = w_gate.shape
    half = rows // 2
    size = min(TAIL, half // 32 * 16 + 16)
    whole = pltpu.VMEM((n * rows, columns), jnp.bfloat16)
    tail = pltpu.VMEM((size, columns), jnp.bfloat16)
    line = pltpu.VMEM((1, columns), jnp.float32)
    anywhere = pl.BlockSpec(memory_space=pl.ANY)
    near = pl.BlockSpec(memory_space=pltpu.VMEM)
    return pl.pallas_call(
        functools.partial(serve_kernel, n, size),
        out_shape=(whole, whole, line, line, tail, tail),
        in_specs=[near] + [anywhere] * 4,
        out_specs=(near,) * 6,
        scratch_shapes=[
            pltpu.VMEM((2, rows, columns), jnp.float32),
            pltpu.VMEM((2, rows, columns), jnp.float32),
            pltpu.VMEM((2, EARLY, columns), jnp.float32),
            pltpu.VMEM((rows, 128), jnp.float32),
            pltpu.VMEM((2, 1, columns), jnp.float32),
            pltpu.VMEM((2, n - 1, 1, columns), jnp.float32),
            pltpu.SemaphoreType.DMA((6,)),
            pltpu.SemaphoreType.DMA((2,)),
            pltpu.SemaphoreType.DMA((2,)),
            pltpu.SemaphoreType.DMA((2,)),
            pltpu.SemaphoreType.DMA((2,)),
            pltpu.SemaphoreType.DMA((2,)),
            pltpu.SemaphoreType.DMA((2, n - 1, 4)),
        ],
        compiler_params=pltpu.CompilerParams(
            collective_id=0, has_side_effects=True, vmem_limit_bytes=VMEM_LIMIT
        ),
        name="serve",
    )(norm_gain, w_gate, avg_gate, w_up, avg_up)


def keep_kernel(parts, gate_ref, up_ref, fg_ref, fu_ref, go_ref, uo_ref, fgo_ref, fuo_ref, lines, sem, line_sem):
    size = gate_ref.shape[0] // parts
    for c in range(parts):
        at = pl.ds(c * size, size)
        for k, (src, dst) in enumerate(((gate_ref, go_ref), (up_ref, uo_ref))):
            pltpu.make_async_copy(src.at[at], dst.at[at], sem.at[k]).start()
    for k, (src, dst) in enumerate(((fg_ref, fgo_ref), (fu_ref, fuo_ref))):
        lines[k][...] = src[0]
        pltpu.make_async_copy(lines[k], dst, line_sem.at[k]).start()
    for k, (ref, out, line) in enumerate(((gate_ref, go_ref, fgo_ref), (up_ref, uo_ref, fuo_ref))):
        pltpu.make_async_copy(ref, out, sem.at[k]).wait()
        pltpu.make_async_copy(lines[k], line, line_sem.at[k]).wait()


def keep(gate, up, factor_gate, factor_up):
    parts = KEEP
    columns = gate.shape[1]
    whole = jax.ShapeDtypeStruct(gate.shape, gate.dtype)
    line = jax.ShapeDtypeStruct((columns,), factor_gate.dtype)
    near = pl.BlockSpec(memory_space=pltpu.VMEM)
    anywhere = pl.BlockSpec(memory_space=pl.ANY)
    return pl.pallas_call(
        functools.partial(keep_kernel, parts),
        out_shape=(whole, whole, line, line),
        in_specs=[near] * 4,
        out_specs=(anywhere,) * 4,
        scratch_shapes=[
            [pltpu.VMEM((columns,), jnp.float32)] * 2,
            pltpu.SemaphoreType.DMA((2,)),
            pltpu.SemaphoreType.DMA((2,)),
        ],
        compiler_params=pltpu.CompilerParams(vmem_limit_bytes=2**20),
        cost_estimate=pl.CostEstimate(flops=100 * gate.size, bytes_accessed=4 * gate.size, transcendentals=0),
        name="keep",
    )(gate, up, factor_gate, factor_up)


def close_kernel(n, way, tail_ref, in_ref, out_ref, sem):
    place = ring_place(lax.axis_index("rows"), n)
    rows = out_ref.shape[0] // n
    first = ring_row((place + (1, n - 1)[way]) % n, n) * rows + way * (rows // 2)
    at = pl.ds(pl.multiple_of(first, 16), tail_ref.shape[0])
    copy = pltpu.make_async_copy(tail_ref, out_ref.at[at], sem)
    copy.start()
    copy.wait()


def close(n, way, tail, gate):
    near = pl.BlockSpec(memory_space=pltpu.VMEM)
    anywhere = pl.BlockSpec(memory_space=pl.ANY)
    return pl.pallas_call(
        functools.partial(close_kernel, n, way),
        out_shape=jax.ShapeDtypeStruct(gate.shape, gate.dtype),
        in_specs=[near, anywhere],
        out_specs=anywhere,
        scratch_shapes=[pltpu.SemaphoreType.DMA],
        input_output_aliases={1: 0},
        compiler_params=pltpu.CompilerParams(vmem_limit_bytes=2**20),
        name="close",
    )(pltpu.with_memory_space_constraint(tail, pltpu.VMEM), gate)


def local(n, w_gate, avg_gate, w_up, avg_up, norm_gain):
    gate, up, factor_gate, factor_up, ahead, back = serve(w_gate, avg_gate, w_up, avg_up, norm_gain, n)
    ring = [ring_row(p, n) for p in range(n)]
    pairs = [(ring[p], ring[(p + 1) % n]) for p in range(n)]
    ahead = lax.ppermute(ahead, "rows", pairs)
    back = lax.ppermute(back, "rows", [(b, a) for a, b in pairs])
    gate, up, factor_gate, factor_up = keep(gate, up, factor_gate, factor_up)
    return (close(n, 1, back, close(n, 0, ahead, gate)), up, factor_gate, factor_up)


def solution(mesh):
    placed = (P("rows", "width"),) * 4 + (P("rows"),)
    return jax.shard_map(
        functools.partial(local, mesh.shape["rows"]),
        mesh=mesh,
        in_specs=placed,
        out_specs=(P(None, "width"), P(None, "width"), P("width"), P("width")),
        check_vma=False,
    )
```
